32 devices in a mesh: dp: 4 (over y, x), fsdp: 8 (over z, core).
Axes of the slice: x: 2, y: 2, z: 4, core: 2. Of those that a mesh axis runs over, the one named last changes fastest.
Arguments:
- latent: bfloat16 [32, 1024, 320], P(('dp', 'fsdp')), may hold values from -6 to 6
- hint: bfloat16 [32, 1024, 320], P(('dp', 'fsdp')), may hold values from -48 to 48
- timestep: int32 [32], P(('dp', 'fsdp')), may hold values from 0 to 999
- skip_grad: bfloat16 [32, 1024, 320], P(('dp', 'fsdp')), may hold values from -6 to 6
- frozen_one: bfloat16 [2880, 320], P('fsdp'), may hold values from -0.109375 to 0.109375
- frozen_two: bfloat16 [2880, 320], P('fsdp'), may hold values from -0.109375 to 0.109375
- time_weight: bfloat16 [320, 1280], P('fsdp'), may hold values from -0.3125 to 0.3125
- frozen_emb: bfloat16 [1280, 320], P('fsdp'), may hold values from -0.15625 to 0.15625
- train_one: bfloat16 [2880, 320], P('fsdp'), may hold values from -0.109375 to 0.109375
- train_two: bfloat16 [2880, 320], P('fsdp'), may hold values from -0.109375 to 0.109375
- train_emb: bfloat16 [1280, 320], P('fsdp'), may hold values from -0.15625 to 0.15625
- zero_weight: bfloat16 [320, 320], P('fsdp'), may hold values from -0.3125 to 0.3125
Outputs:
- skip: bfloat16 [32, 1024, 320], P(('dp', 'fsdp'))
- grad_one: float32 [2880, 320], P('fsdp')
- grad_two: float32 [2880, 320], P('fsdp')
- grad_emb: float32 [1280, 320], P('fsdp')
- grad_zero: float32 [320, 320], P('fsdp')
- grad_norm: float32 [], replicated
The draws below stay inside these ranges and needn't reach their ends.
All inputs are finite; a program needn't handle non-finite values.
Results may differ from the reference program's by a relative error of at most 0.018.
Values may be sent and summed in bfloat16 or wider, within the bound.
No kernel may reach another device: no remote copies, remote signals or barrier semaphores. Data moves between devices by JAX's collectives and lax.ppermute only.
A program may use at most 128 MiB of HBM per device.

```python
import math
import jax
import jax.numpy as jnp
from jax import lax

C = 320
TEMB = 1280
COLS = 64
POS = 1024
BATCH = 32


def draw_hint(key, part):
    key = jax.random.fold_in(key, 7311)
    ramp = jnp.arange(C).astype(jnp.float32) / (C - 1)
    scales = jnp.exp(jnp.log(8.0) * ramp)
    noise = jnp.clip(jax.random.normal(key, (BATCH, POS, C), jnp.float32), -6.0, 6.0)
    values = noise * scales[None, None, :]
    return jnp.clip(values, -48.0, 48.0).astype(jnp.bfloat16)


def plant(drawn, key, least, top_value):
    spot = [jax.random.randint(jax.random.fold_in(key, axis), (), 0, length) for axis, length in enumerate(drawn.shape)]
    main_axis = drawn.shape.index(max(drawn.shape))
    next_to = spot[:main_axis] + [(spot[main_axis] + 1) % drawn.shape[main_axis]] + spot[main_axis + 1:]
    return drawn.at[tuple(spot)].set(least).at[tuple(next_to)].set(top_value)


def steps_of(stream_key, dims, cuts, smallest, top_value):
    def one(position, blocks):
        draws = jax.random.uniform(jax.random.fold_in(jax.random.fold_in(stream_key, 6), position), (blocks,), jnp.float32, smallest / len(cuts), top_value / len(cuts))
        return jnp.repeat(jnp.exp(draws), dims[position] // blocks).reshape((-1,) + (1,) * (len(dims) - position - 1))

    factor_of = one(*cuts[0])
    for cut in cuts[1:]:
        factor_of = factor_of * one(*cut)
    return factor_of


def centred(key, extent, deviation, most, pieces=(), kind=jnp.bfloat16):
    factor_of = steps_of(key, extent, pieces, -0.22, 0.18) if pieces else 1.0
    result = jax.random.normal(key, extent, jnp.float32) * deviation * factor_of
    return jnp.minimum(jnp.maximum(result, -most), most).astype(kind)


def setup_inputs(seed: int = 0) -> dict:
    splits = jax.random.split(jax.random.key(seed), 13)
    return {
        "latent": centred(splits[0], (BATCH, POS, C), 1.0, 6.0, ((0, 32),)),
        "hint": draw_hint(jax.random.fold_in(splits[12], 71), 0),
        "timestep": plant(jax.random.randint(splits[2], (BATCH,), 0, 1000), jax.random.fold_in(splits[2], 1), 0, 999).astype(jnp.int32),
        "skip_grad": centred(splits[3], (BATCH, POS, C), 1.0, 6.0, ((0, 32),)),
        "frozen_one": centred(splits[4], (9 * C, C), (9 * C) ** -0.5, 0.109375, ((0, 8),)),
        "frozen_two": centred(splits[5], (9 * C, C), (9 * C) ** -0.5, 0.109375, ((0, 8),)),
        "time_weight": centred(splits[6], (C, TEMB), C ** -0.5, 0.3125, ((0, 8),)),
        "frozen_emb": centred(splits[7], (TEMB, C), TEMB ** -0.5, 0.15625, ((0, 8),)),
        "train_one": centred(splits[8], (9 * C, C), (9 * C) ** -0.5, 0.109375, ((0, 8),)),
        "train_two": centred(splits[9], (9 * C, C), (9 * C) ** -0.5, 0.109375, ((0, 8),)),
        "train_emb": centred(splits[10], (TEMB, C), TEMB ** -0.5, 0.15625, ((0, 8),)),
        "zero_weight": centred(splits[11], (C, C), C ** -0.5, 0.3125, ((0, 8),)),
    }


group_count = 32
clip_limit = 1.0

def conv_apply(flat, kernel):
    count, chans = flat.shape
    height = count // COLS
    padded = jnp.pad(flat.reshape(height, COLS, chans), ((1, 1), (1, 1), (0, 0)))
    total = jnp.zeros((count, kernel.shape[1]), jnp.float32)
    for offset in range(9):
        row_off = offset // 3
        col_off = offset % 3
        piece = padded[row_off:row_off + height, col_off:col_off + COLS].reshape(count, chans)
        total = total + jnp.dot(piece, kernel[offset * chans:(offset + 1) * chans], preferred_element_type=jnp.float32)
    return total

def conv_back(flat, kernel):
    count, chans = flat.shape
    height = count // COLS
    inner = kernel.shape[0] // 9
    padded = jnp.pad(flat.reshape(height, COLS, chans), ((1, 1), (1, 1), (0, 0)))
    total = jnp.zeros((count, inner), jnp.float32)
    for offset in range(9):
        row_off = offset // 3
        col_off = offset % 3
        piece = padded[2 - row_off:2 - row_off + height, 2 - col_off:2 - col_off + COLS].reshape(count, chans)
        block = kernel[offset * inner:(offset + 1) * inner]
        total = total + lax.dot_general(piece, block, (((1,), (1,)), ((), ())), preferred_element_type=jnp.float32)
    return total

def conv_grads(flat, upstream):
    count, chans = flat.shape
    height = count // COLS
    padded = jnp.pad(flat.reshape(height, COLS, chans), ((1, 1), (1, 1), (0, 0)))
    blocks = []
    for offset in range(9):
        row_off = offset // 3
        col_off = offset % 3
        piece = padded[row_off:row_off + height, col_off:col_off + COLS].reshape(count, chans)
        blocks.append(lax.dot_general(piece, upstream, (((0,), (0,)), ((), ())), preferred_element_type=jnp.float32))
    return jnp.concatenate(blocks, axis=0)

def group_norm(value):
    count, chans = value.shape
    grouped = value.reshape(count, group_count, chans // group_count)
    center = lax.optimization_barrier(jnp.mean(grouped, axis=(0, 2), keepdims=True))
    spread = lax.optimization_barrier(jnp.mean((grouped - center) ** 2, axis=(0, 2), keepdims=True))
    inverse = lax.rsqrt(spread + 1e-05)
    return (((grouped - center) * inverse).reshape(count, chans), inverse)

def norm_back(upstream, normed, inverse):
    count, chans = upstream.shape
    grouped = upstream.reshape(count, group_count, chans // group_count)
    shaped = normed.reshape(count, group_count, chans // group_count)
    first = lax.optimization_barrier(jnp.mean(grouped, axis=(0, 2), keepdims=True))
    second = lax.optimization_barrier(jnp.mean(grouped * shaped, axis=(0, 2), keepdims=True))
    return ((grouped - first - shaped * second) * inverse).reshape(count, chans)

def time_embed(timestep, time_weight):
    half = time_weight.shape[0] // 2
    freqs = jnp.exp(-math.log(10000.0) * jnp.arange(half).astype(jnp.float32) / half)
    angles = timestep.astype(jnp.float32)[:, None] * freqs[None, :]
    wave = jnp.concatenate([jnp.cos(angles), jnp.sin(angles)], axis=1).astype(jnp.bfloat16)
    return jax.nn.silu(jnp.dot(wave, time_weight, preferred_element_type=jnp.float32)).astype(jnp.bfloat16)

def sample_step(latent_one, hint_one, cotangent, emb_one, weights):
    frozen_one, frozen_two, frozen_emb, train_one, train_two, train_emb, zero_weight = weights
    base = latent_one.astype(jnp.float32)
    emb_row = emb_one[None, :]
    fa0 = jax.nn.silu(group_norm(base)[0]).astype(jnp.bfloat16)
    fp1 = conv_apply(fa0, frozen_one) + jnp.dot(emb_row, frozen_emb, preferred_element_type=jnp.float32)
    fa1 = jax.nn.silu(group_norm(fp1)[0]).astype(jnp.bfloat16)
    frozen_out = base + conv_apply(fa1, frozen_two)
    mixed_in = base + hint_one.astype(jnp.float32)
    a_zero = jax.nn.silu(group_norm(mixed_in)[0]).astype(jnp.bfloat16)
    p_one = conv_apply(a_zero, train_one) + jnp.dot(emb_row, train_emb, preferred_element_type=jnp.float32)
    y_one, inverse = group_norm(p_one)
    a_one = jax.nn.silu(y_one).astype(jnp.bfloat16)
    control = (mixed_in + conv_apply(a_one, train_two)).astype(jnp.bfloat16)
    skip_one = (frozen_out + jnp.dot(control, zero_weight, preferred_element_type=jnp.float32)).astype(jnp.bfloat16)
    grad_z = lax.dot_general(control, cotangent, (((0,), (0,)), ((), ())), preferred_element_type=jnp.float32)
    d_control = lax.dot_general(cotangent, zero_weight, (((1,), (1,)), ((), ())), preferred_element_type=jnp.float32).astype(jnp.bfloat16)
    grad_w2 = conv_grads(a_one, d_control)
    d_aone = conv_back(d_control, train_two)
    sig = jax.nn.sigmoid(y_one)
    d_yone = d_aone * sig * (1.0 + y_one * (1.0 - sig))
    d_pone = norm_back(d_yone, y_one, inverse)
    grad_e = emb_one.astype(jnp.float32)[:, None] * lax.optimization_barrier(jnp.sum(d_pone, axis=0))[None, :]
    grad_w1 = conv_grads(a_zero, d_pone.astype(jnp.bfloat16))
    return (skip_one, (grad_w1, grad_w2, grad_e, grad_z))

def run_batch(latent, hint, skip_grad, emb, weights):
    train_one, train_emb, zero_weight = (weights[3], weights[5], weights[6])
    start = (jnp.zeros(train_one.shape, jnp.float32), jnp.zeros(train_one.shape, jnp.float32), jnp.zeros(train_emb.shape, jnp.float32), jnp.zeros(zero_weight.shape, jnp.float32))

    def advance(carry, items):
        skip_one, grads = sample_step(items[0], items[1], items[2], items[3], weights)
        return (tuple((old + new for old, new in zip(carry, grads))), skip_one)
    grads, skips = lax.scan(advance, start, (latent, hint, skip_grad, emb))
    return (skips, grads)

def reference(latent, hint, timestep, skip_grad, frozen_one, frozen_two, time_weight, frozen_emb, train_one, train_two, train_emb, zero_weight):
    emb = time_embed(timestep, time_weight)
    weights = (frozen_one, frozen_two, frozen_emb, train_one, train_two, train_emb, zero_weight)
    skips, grads = run_batch(latent, hint, skip_grad, emb, weights)
    total = sum((jnp.sum(item * item) for item in grads))
    grad_norm = jnp.sqrt(total + 1e-06)
    scale = jnp.minimum(1.0, clip_limit / grad_norm)
    return (skips, grads[0] * scale, grads[1] * scale, grads[2] * scale, grads[3] * scale, grad_norm)
```

```python
import math
import jax
import jax.numpy as jnp
from jax import lax
from jax.experimental import pallas as pl
from jax.experimental.pallas import tpu as pltpu
from jax.sharding import PartitionSpec as P

COLS = 64
GROUPS = 32
BF = jnp.bfloat16
F32 = jnp.float32
VMEM_MB = 44
AXES = ("dp", "fsdp")


def call(kernel, outs, scratch=(), flops=0, n_smem=0, n_in=0, name=None):
    vm = pl.BlockSpec(memory_space=pltpu.VMEM)
    sm = pl.BlockSpec(memory_space=pltpu.SMEM)
    return pl.pallas_call(
        kernel,
        out_shape=[jax.ShapeDtypeStruct(s, d) for s, d in outs],
        in_specs=[sm] * n_smem + [vm] * n_in,
        out_specs=[vm] * len(outs),
        scratch_shapes=[pltpu.VMEM(s, d) for s, d in scratch],
        compiler_params=pltpu.CompilerParams(vmem_limit_bytes=VMEM_MB << 20),
        cost_estimate=pl.CostEstimate(flops=flops, bytes_accessed=0, transcendentals=0),
        name=name,
    )


def group_mix(chans, count):
    per = chans // GROUPS
    mul = (1 << 16) // per + 1
    row = (lax.broadcasted_iota(jnp.int32, (chans, chans), 0) * mul) >> 16
    col = (lax.broadcasted_iota(jnp.int32, (chans, chans), 1) * mul) >> 16
    return jnp.where(row == col, 1.0 / (per * count), 0.0).astype(F32)


def fold(block):
    return block.reshape(block.shape[0] // 8, 8, block.shape[1]).sum(axis=0)


def mix_rows(part, mix):
    total = jnp.sum(part, axis=0, keepdims=True)
    wide = jnp.broadcast_to(total, part.shape)
    return jnp.dot(wide, mix, precision=lax.Precision.HIGHEST, preferred_element_type=F32)[0:1]


def stats(read, count, chans, mix):
    rows = count // COLS
    zero = jnp.zeros((8, chans), F32)
    tot = lax.fori_loop(0, rows, lambda i, a: a + fold(read(i)), zero)
    mean = mix_rows(tot, mix)

    def dev(i, a):
        d = read(i) - mean
        return a + fold(d * d)

    var = mix_rows(lax.fori_loop(0, rows, dev, zero), mix)
    return mean, lax.rsqrt(var + 1e-05)


def rows_of(ref, i, lead=0):
    return ref[pl.ds(pl.multiple_of(i * COLS + lead, COLS), COLS), :]


def spread(p_ref, i, block):
    chans = block.shape[1]
    pos = lax.broadcasted_iota(jnp.int32, block.shape, 0)
    left = jnp.where(pos == 0, 0.0, pltpu.roll(block, 1, 0))
    right = jnp.where(pos == COLS - 1, 0.0, pltpu.roll(block, COLS - 1, 0))
    at = pl.ds(pl.multiple_of(i * COLS + COLS, COLS), COLS)
    p_ref[at, :] = jnp.concatenate([left, block, right], axis=1).astype(BF)


def edge_zero(p_ref):
    n, c = p_ref.shape
    p_ref[0:COLS, :] = jnp.zeros((COLS, c), BF)
    p_ref[n - COLS : n, :] = jnp.zeros((COLS, c), BF)


def conv(p_ref, w_ref, count):
    k = p_ref.shape[1]
    out = None
    for a in range(3):
        d = jnp.dot(p_ref[a * COLS : a * COLS + count, :], w_ref[a * k : (a + 1) * k, :], preferred_element_type=F32)
        out = d if out is None else out + d
    return out


def conv_back(p_ref, w_ref, count):
    k = p_ref.shape[1]
    c = k // 3
    out = None
    for a in range(3):
        for b in range(3):
            blk = w_ref[(3 * a + b) * c : (3 * a + b + 1) * c, :]
            d = lax.dot_general(
                p_ref[(2 - a) * COLS : (2 - a) * COLS + count, (2 - b) * c : (3 - b) * c],
                blk, (((1,), (1,)), ((), ())), preferred_element_type=F32)
            out = d if out is None else out + d
    return out


def t_dot(left, right):
    return lax.dot_general(left, right, (((0,), (0,)), ((), ())), preferred_element_type=F32)


class Plan:
    def __init__(self, rows, dp):
        groups = rows // 8
        self.rows = rows
        self.win = -(-groups // dp) * 8
        self.win += self.win % 16
        self.dp = dp

    def start(self, q):
        span = (self.rows - self.win) // 8
        return (span * q // (self.dp - 1)) * 8


def start_of(plan, q):
    if isinstance(q, int):
        return plan.start(q)
    out = jnp.int32(0)
    for i in range(plan.dp):
        out = jnp.where(q == i, jnp.int32(plan.start(i)), out)
    return out


def gather_in(wf, ids, own, mate, parts, plan, nz):
    dp_i, z_i, c_i = ids
    rows, win = plan.rows, plan.win
    for cc, src in ((0, own), (1, mate)):
        s = 2 * z_i + (c_i ^ cc)
        wf[pl.ds(pl.multiple_of(s * rows, 8), rows), :] = src[...].astype(F32)
    for cc in range(2):
        for d in range(plan.dp):
            at = start_of(plan, dp_i ^ d)
            src = parts[cc * plan.dp + d]
            for j in range(1, nz):
                s = 2 * (z_i ^ j) + (c_i ^ cc)
                wf[pl.ds(pl.multiple_of(s * rows + at, 8), win), :] = src[(j - 1) * win : j * win, :].astype(F32)


def matrix(w_ref, wf, off, per, rows, shards):
    for s in range(shards):
        w_ref[s * per : (s + 1) * per, :] = wf[s * rows + off : s * rows + off + per, :].astype(BF)


def norm_in(ids, lat, hint, pf, p):
    count, chans = lat.shape
    mix = group_mix(chans, count)
    edge_zero(pf)
    edge_zero(p)

    def base(i):
        return rows_of(lat, i).astype(F32)

    def mixed(i):
        return base(i) + rows_of(hint, i).astype(F32)

    for read, out in ((mixed, p), (base, pf)):
        mean, inv = stats(read, count, chans, mix)

        def put(i, _, read=read, out=out, mean=mean, inv=inv):
            spread(out, i, jax.nn.silu((read(i) - mean) * inv))
            return 0

        lax.fori_loop(0, count // COLS, put, 0)


def first_conv(sz, ids, p0, own, mate, *rest):
    parts, (c1, wf, w) = rest[: 2 * sz.dp], rest[2 * sz.dp :]
    where = (ids[0], ids[1], ids[2])
    gather_in(wf, where, own, mate, parts, sz.t1, sz.nz)
    matrix(w, wf, 0, sz.r_conv, sz.t1.rows, sz.shards)
    c1[...] = conv(p0, w, c1.shape[0])


def put_rows(gf, value, base, per, off, rows):
    at, end = base, base + value.shape[0]
    while at < end:
        s = at // per
        stop = min(end, (s + 1) * per)
        to = s * rows + off + at - s * per
        gf[to : to + stop - at, :] = value[at - base : stop - base, :]
        at = stop


def split_cores(gf, keep, send, c_i, rows, nz):
    for z in range(nz):
        for out, c in ((keep, c_i), (send, 1 - c_i)):
            s = 2 * z + c
            out[z * rows : (z + 1) * rows, :] = gf[pl.ds(pl.multiple_of(s * rows, 8), rows), :].astype(BF)


def control_step(sz, ids, c1, lat, hint, cot, wave, own, mate, *rest):
    parts = rest[: 2 * sz.dp]
    (y1, inv_o, pdc, w2, ctl, zw, emb_o, keep, send, wf, te, tw, pa, dcb, gf) = rest[2 * sz.dp :]
    count, chans = c1.shape
    n = count // COLS
    mix = group_mix(chans, count)
    gather_in(wf, (ids[0], ids[1], ids[2]), own, mate, parts, sz.t2, sz.nz)
    per_t = sz.t2.rows
    o1, o2, o3 = sz.r_conv, sz.r_conv + sz.r_zero, sz.r_conv + sz.r_zero + sz.r_emb
    matrix(w2, wf, 0, sz.r_conv, per_t, sz.shards)
    matrix(zw, wf, o1, sz.r_zero, per_t, sz.shards)
    matrix(te, wf, o2, sz.r_emb, per_t, sz.shards)
    blocks = sz.temb // chans
    for j in range(blocks):
        for s in range(sz.shards):
            src = s * per_t + o3 + j * sz.r_time
            tw[j * chans + s * sz.r_time : j * chans + (s + 1) * sz.r_time, :] = wf[src : src + sz.r_time, :].astype(BF)
    pe = jnp.zeros((8, chans), F32)
    for j in range(blocks):
        e = jnp.dot(wave[...], tw[j * chans : (j + 1) * chans, :], preferred_element_type=F32)
        e = jax.nn.silu(e).astype(BF)
        emb_o[:, j * chans : (j + 1) * chans] = e
        pe = pe + jnp.dot(e, te[j * chans : (j + 1) * chans, :], preferred_element_type=F32)
    pe = pe[0:1]

    def read(i):
        return rows_of(c1, i) + pe

    mean, inv = stats(read, count, chans, mix)
    inv_o[...] = jnp.broadcast_to(inv, inv_o.shape)
    edge_zero(pa)
    edge_zero(pdc)

    def act(i, _):
        y = (read(i) - mean) * inv
        at = pl.ds(pl.multiple_of(i * COLS, COLS), COLS)
        y1[at, :] = y
        spread(pa, i, jax.nn.silu(y))
        dc = lax.dot_general(rows_of(cot, i), zw[...], (((1,), (1,)), ((), ())), preferred_element_type=F32)
        dcb[at, :] = dc.astype(BF)
        spread(pdc, i, dc)
        return 0

    lax.fori_loop(0, n, act, 0)
    mixed = lat[...].astype(F32) + hint[...].astype(F32)
    ctl[...] = (mixed + conv(pa, w2, count)).astype(BF)
    rows = sz.g1.rows
    put_rows(gf, t_dot(ctl[...], cot[...]), 0, sz.r_zero, sz.r_conv, rows)
    for a in range(3):
        d = t_dot(pa[a * COLS : a * COLS + count, :], dcb[...])
        put_rows(gf, d, a * 3 * chans, sz.r_conv, 0, rows)
    split_cores(gf, keep, send, ids[2], rows, sz.nz)


def back_step(sz, ids, y1, inv_i, pdc, w2, p0, emb, keep, send, da, dyb, gf):
    count, chans = y1.shape
    n = count // COLS
    mix = group_mix(chans, count)
    inv = inv_i[0:1]
    da[...] = conv_back(pdc, w2, count)
    zero = jnp.zeros((8, chans), F32)

    def grad(i, acc):
        y = rows_of(y1, i)
        sig = jax.nn.sigmoid(y)
        dy = rows_of(da, i) * sig * (1.0 + y * (1.0 - sig))
        da[pl.ds(pl.multiple_of(i * COLS, COLS), COLS), :] = dy
        return acc[0] + fold(dy), acc[1] + fold(dy * y)

    s1, s2 = lax.fori_loop(0, n, grad, (zero, zero))
    m1, m2 = mix_rows(s1, mix), mix_rows(s2, mix)

    def fin(i, acc):
        d = (rows_of(da, i) - m1 - rows_of(y1, i) * m2) * inv
        dyb[pl.ds(pl.multiple_of(i * COLS, COLS), COLS), :] = d.astype(BF)
        return acc + fold(d)

    dsum = jnp.sum(lax.fori_loop(0, n, fin, zero), axis=0, keepdims=True)
    rows = sz.g2.rows
    for a in range(3):
        d = t_dot(p0[a * COLS : a * COLS + count, :], dyb[...])
        put_rows(gf, d, a * 3 * chans, sz.r_conv, 0, rows)
    split_cores(gf, keep, send, ids[2], rows, sz.nz)
    vec = jnp.zeros((sz.vr, chans), F32)
    line = lax.broadcasted_iota(jnp.int32, vec.shape, 0)
    for s in range(sz.shards):
        e = emb[0:1, s * sz.r_emb : (s + 1) * sz.r_emb].astype(F32)
        if sz.r_emb < chans:
            e = jnp.concatenate([e, jnp.zeros((1, chans - sz.r_emb), F32)], axis=1)
        vec = jnp.where(line == s, e, vec)
    vec = jnp.where(line == sz.shards, dsum, vec)
    for out in (keep, send):
        out[sz.nz * rows :, :] = vec.astype(BF)


def frozen_step(sz, pf, emb, lat, ctl, zw, ids, own, mate, *rest):
    parts = rest[: 2 * sz.dp]
    skip, wf, w1, w2, fe, pa, c1 = rest[2 * sz.dp :]
    count, chans = lat.shape
    n = count // COLS
    mix = group_mix(chans, count)
    gather_in(wf, (ids[0], ids[1], ids[2]), own, mate, parts, sz.fz, sz.nz)
    matrix(w1, wf, 0, sz.r_conv, sz.fz.rows, sz.shards)
    matrix(w2, wf, sz.r_conv, sz.r_conv, sz.fz.rows, sz.shards)
    matrix(fe, wf, 2 * sz.r_conv, sz.r_emb, sz.fz.rows, sz.shards)
    pe = jnp.dot(emb[...], fe[...], preferred_element_type=F32)[0:1]
    c1[...] = conv(pf, w1, count)

    def read(i):
        return rows_of(c1, i) + pe

    mean, inv = stats(read, count, chans, mix)
    edge_zero(pa)

    def act(i, _):
        spread(pa, i, jax.nn.silu((read(i) - mean) * inv))
        return 0

    lax.fori_loop(0, n, act, 0)
    out = lat[...].astype(F32) + conv(pa, w2, count)
    skip[...] = (out + jnp.dot(ctl[...], zw[...], preferred_element_type=F32)).astype(BF)


def tree(values):
    while len(values) > 1:
        values = [values[i] + values[i + 1] for i in range(0, len(values), 2)]
    return values[0]


def add_cores(sz, plan, vec, ids, keep, got, *rest):
    msgs, (hf,) = rest[: sz.dp], rest[sz.dp :]
    body = sz.nz * plan.rows
    hf[...] = keep[0:body, :].astype(F32) + got[0:body, :].astype(F32)
    for d in range(sz.dp):
        at = start_of(plan, ids[0] ^ d)
        for z in range(sz.nz):
            src = pl.ds(pl.multiple_of(z * plan.rows + at, 8), plan.win)
            msgs[d][z * plan.win : (z + 1) * plan.win, :] = hf[src, :].astype(BF)
    if vec:
        mine, other = keep[body:, :].astype(F32), got[body:, :].astype(F32)
        first = ids[2] == 0
        both = (jnp.where(first, mine, other), jnp.where(first, other, mine))
        for m in msgs:
            for i, v in enumerate(both):
                at = sz.nz * plan.win + i * sz.vr
                m[at : at + sz.vr, :] = v.astype(BF)


def add_dp(sz, plan, vec, ids, *refs):
    got, msgs, scr = refs[: sz.dp], refs[sz.dp : sz.dp + sz.nz], refs[sz.dp + sz.nz :]
    body = sz.nz * plan.win
    xf = scr[0]
    xf[...] = tree([g[0:body, :].astype(F32) for g in got])
    if vec:
        vf = scr[1]
        span = 2 * sz.vr
        for d in range(sz.dp):
            at = pl.multiple_of((ids[0] ^ d) * span, 8)
            vf[pl.ds(at, span), :] = got[d][body:, :].astype(F32)
    for j in range(sz.nz):
        z = ids[1] ^ j
        msgs[j][0 : plan.win, :] = xf[pl.ds(pl.multiple_of(z * plan.win, 8), plan.win), :].astype(BF)
        if vec:
            s = 2 * z + ids[2]
            vs = [vf[pl.ds(i * sz.vr + s, 1), :] for i in range(2 * sz.dp)]
            vs += [vf[i * sz.vr + sz.shards : i * sz.vr + sz.shards + 1, :] for i in range(2 * sz.dp)]
            msgs[j][plan.win :, :] = jnp.concatenate(vs, axis=0).astype(BF)


def add_z(sz, plan, vec, ids, *refs):
    got = refs[: sz.nz]
    outs = refs[sz.nz :]
    outs[0][...] = tree([g[0 : plan.win, :].astype(F32) for g in got]).astype(BF)
    if vec:
        de, ev = outs[1], outs[2]
        span = 4 * sz.dp
        for j in range(sz.nz):
            ev[pl.ds(pl.multiple_of((ids[1] ^ j) * span, 8), span), :] = got[j][plan.win :, :].astype(F32)
        half = 2 * sz.dp
        e = jnp.concatenate([ev[z * span : z * span + half, :] for z in range(sz.nz)], axis=0)
        d = jnp.concatenate([ev[z * span + half : (z + 1) * span, :] for z in range(sz.nz)], axis=0)
        de[...] = t_dot(e, d)[0 : de.shape[0]]


def whole_shard(sz, plan, ids, got, out):
    line = lax.broadcasted_iota(jnp.int32, (plan.win, out.shape[1]), 0)
    for d in range(sz.dp):
        q = ids[0] ^ d
        at = start_of(plan, q)
        stop = jnp.where(q == sz.dp - 1, jnp.int32(plan.rows), start_of(plan, q + 1))
        here = pl.ds(pl.multiple_of(at, 8), plan.win)
        out[here, :] = jnp.where(line < stop - at, got[d][...].astype(F32), out[here, :])


def square(x):
    return jnp.sum(fold(x * x), axis=0, keepdims=True) if x.shape[0] % 8 == 0 else jnp.sum(x * x, axis=0, keepdims=True)


def collect(sz, ids, *refs):
    g1, g2 = refs[: sz.dp], refs[sz.dp : 2 * sz.dp]
    de, own1, own2, part = refs[2 * sz.dp :]
    own1[...] = jnp.zeros(own1.shape, F32)
    own2[...] = jnp.zeros(own2.shape, F32)
    whole_shard(sz, sz.g1, ids, g1, own1)
    whole_shard(sz, sz.g2, ids, g2, own2)
    total = square(own1[...]) + square(own2[...]) + square(de[...])
    part[...] = jnp.broadcast_to(jnp.sum(total, axis=1, keepdims=True), part.shape)


def finish(sz, own1, own2, de, part, *refs):
    mate = refs[0]
    one, two, emb, zero, norm = refs[1:]
    total = part[...] + mate[...]
    root = jnp.sqrt(total + 1e-06)
    norm[...] = root
    scale = jnp.minimum(1.0, 1.0 / root)[0:1, 0:1]
    one[...] = own2[0 : one.shape[0], :] * scale
    two[...] = own1[0 : two.shape[0], :] * scale
    zero[...] = own1[sz.r_conv : sz.r_conv + zero.shape[0], :] * scale
    emb[...] = de[...] * scale


def add_parts(*refs):
    refs[-1][...] = tree([r[...] for r in refs[:-1]])


class Sizes:
    pass


def up8(x):
    return -(-x // 8) * 8


def solution(mesh):
    dp, shards = mesh.shape["dp"], mesh.shape["fsdp"]
    nz = shards // 2

    def coords(i):
        return i // shards, (i % shards) // 2, i % 2

    def perm(d, z, c):
        out = []
        for i in range(dp * shards):
            a, b, e = coords(i)
            out.append((i, (a ^ d) * shards + 2 * (b ^ z) + (e ^ c)))
        return out

    def pp(x, d=0, z=0, c=0):
        return lax.ppermute(x, AXES, perm(d, z, c))

    def body(latent, hint, timestep, skip_grad, frozen_one, frozen_two, time_weight,
             frozen_emb, train_one, train_two, train_emb, zero_weight):
        count, chans = latent.shape[1:]
        sz = Sizes()
        sz.dp, sz.nz, sz.shards = dp, nz, shards
        sz.r_conv, sz.r_zero, sz.r_emb = train_one.shape[0], zero_weight.shape[0], train_emb.shape[0]
        sz.r_time, sz.temb = time_weight.shape
        sz.vr = -(-(shards + 1) // 16) * 16
        blocks = sz.temb // chans

        def pack(arrays):
            x = jnp.concatenate(arrays, axis=0) if len(arrays) > 1 else arrays[0]
            extra = up8(x.shape[0]) - x.shape[0]
            return jnp.pad(x, ((0, extra), (0, 0))) if extra else x

        tw = [time_weight[:, j * chans : (j + 1) * chans] for j in range(blocks)]
        b1 = pack([train_one])
        b2 = pack([train_two, zero_weight, train_emb] + tw)
        b3 = pack([frozen_one, frozen_two, frozen_emb])
        sz.t1, sz.t2, sz.fz = Plan(b1.shape[0], dp), Plan(b2.shape[0], dp), Plan(b3.shape[0], dp)
        sz.g1, sz.g2 = Plan(up8(sz.r_conv + sz.r_zero), dp), Plan(up8(sz.r_conv), dp)
        dp_i = lax.axis_index("dp")
        f_i = lax.axis_index("fsdp")
        ids = jnp.stack([dp_i, f_i // 2, f_i % 2]).astype(jnp.int32)

        def gather(shard, plan):
            q0 = lax.dynamic_slice_in_dim(shard, start_of(plan, dp_i), plan.win, 0)
            mate = pp(shard, c=1)
            s = jnp.concatenate([pp(q0, z=j) for j in range(1, nz)], axis=0)
            sd = [s] + [pp(s, d=d) for d in range(1, dp)]
            return [shard, mate] + sd + [pp(x, c=1) for x in sd]

        import functools as ft
        pad = count + 2 * COLS
        wide = 3 * chans
        conv_rows = sz.r_conv * shards
        lat, hin, cot = latent[0], hint[0], skip_grad[0]
        pf0, p0 = call(norm_in, [((pad, wide), BF)] * 2, n_smem=1, n_in=2, flops=10**9, name="norm_in")(ids, lat, hin)
        a1 = gather(b1, sz.t1)
        a2 = gather(b2, sz.t2)
        a3 = gather(b3, sz.fz)
        mm = 2 * count * conv_rows * chans
        (c1,) = call(ft.partial(first_conv, sz), [((count, chans), F32)],
                     [((shards * sz.t1.rows, chans), F32), ((conv_rows, chans), BF)],
                     n_smem=1, n_in=1 + len(a1), flops=mm, name="first_conv")(ids, p0, *a1)
        half = sz.r_time * shards // 2
        freqs = jnp.exp(-math.log(10000.0) * jnp.arange(half).astype(F32) / half)
        angles = timestep.astype(F32)[:, None] * freqs[None, :]
        wave = jnp.concatenate([jnp.cos(angles), jnp.sin(angles)], axis=1).astype(BF)
        wave = jnp.broadcast_to(wave, (8, wave.shape[1]))
        g1r, g2r = nz * sz.g1.rows, nz * sz.g2.rows + sz.vr
        y1, inv, pdc, w2, ctl, zw, emb, keep1, send1 = call(
            ft.partial(control_step, sz),
            [((count, chans), F32), ((8, chans), F32), ((pad, wide), BF), ((conv_rows, chans), BF),
             ((count, chans), BF), ((chans, chans), BF), ((8, sz.temb), BF), ((g1r, chans), BF), ((g1r, chans), BF)],
            [((shards * sz.t2.rows, chans), F32), ((sz.temb, chans), BF), ((sz.temb, chans), BF),
             ((pad, wide), BF), ((count, chans), BF), ((shards * sz.g1.rows, chans), F32)],
            n_smem=1, n_in=5 + len(a2), flops=2 * mm, name="control_step")(ids, c1, lat, hin, cot, wave, *a2)
        keep2, send2 = call(
            ft.partial(back_step, sz), [((g2r, chans), BF)] * 2,
            [((count, chans), F32), ((count, chans), BF), ((shards * sz.g2.rows, chans), F32)],
            n_smem=1, n_in=6, flops=2 * mm, name="back_step")(ids, y1, inv, pdc, w2, p0, emb)
        (skip,) = call(
            ft.partial(frozen_fix, sz), [((count, chans), BF)],
            [((shards * sz.fz.rows, chans), F32), ((conv_rows, chans), BF), ((conv_rows, chans), BF),
             ((sz.temb, chans), BF), ((pad, wide), BF), ((count, chans), F32)],
            n_smem=1, n_in=5 + len(a3), flops=2 * mm, name="frozen_step")(ids, pf0, emb, lat, ctl, zw, *a3)

        def reduce(keep, send, plan, vec, tag):
            got = pp(send, c=1)
            msg = ((nz * plan.win + (2 * sz.vr if vec else 0), chans), BF)
            ms = call(ft.partial(add_cores, sz, plan, vec), [msg] * dp,
                      [((nz * plan.rows, chans), F32)], n_smem=1, n_in=2, name=tag + "_cores")(ids, keep, got)
            ms = [ms[0]] + [pp(ms[d], d=d) for d in range(1, dp)]
            zmsg = ((plan.win + (4 * dp if vec else 0), chans), BF)
            scr = [((nz * plan.win, chans), F32)] + ([((dp * 2 * sz.vr, chans), F32)] if vec else [])
            zs = call(ft.partial(add_dp, sz, plan, vec), [zmsg] * nz, scr,
                      n_smem=1, n_in=dp, name=tag + "_dp")(ids, *ms)
            zs = [zs[0]] + [pp(zs[j], z=j) for j in range(1, nz)]
            outs = [((plan.win, chans), BF)] + ([((sz.r_emb, chans), F32)] if vec else [])
            scr = [((nz * 4 * dp, chans), F32)] if vec else []
            res = call(ft.partial(add_z, sz, plan, vec), outs, scr, n_smem=1, n_in=nz, name=tag + "_z")(ids, *zs)
            own = res[0]
            return [own] + [pp(own, d=d) for d in range(1, dp)], (res[1] if vec else None)

        r1, _ = reduce(keep1, send1, sz.g1, False, "two")
        r2, de = reduce(keep2, send2, sz.g2, True, "one")
        own1, own2, part = call(
            ft.partial(collect, sz), [((sz.g1.rows, chans), F32), ((sz.g2.rows, chans), F32), ((8, 128), F32)],
            n_smem=1, n_in=2 * dp + 1, name="collect")(ids, *r1, *r2, de)
        parts = [part] + [pp(part, z=j) for j in range(1, nz)]
        (part,) = call(add_parts, [((8, 128), F32)], n_in=nz, name="add_parts")(*parts)
        mate = pp(part, c=1)
        one, two, ge, gz, norm = call(
            ft.partial(finish, sz),
            [((sz.r_conv, chans), F32), ((sz.r_conv, chans), F32), ((sz.r_emb, chans), F32),
             ((sz.r_zero, chans), F32), ((8, 128), F32)],
            n_in=5, name="finish")(own1, own2, de, part, mate)
        return skip[None], one, two, ge, gz, norm[0, 0]

    row = P("fsdp", None)
    big = P(AXES, None, None)
    in_specs = (big, big, P(AXES), big) + (row,) * 8
    out_specs = (big, row, row, row, row, P())
    return jax.shard_map(body, mesh=mesh, in_specs=in_specs, out_specs=out_specs, check_vma=False)


def frozen_fix(sz, ids, pf, emb, lat, ctl, zw, *rest):
    frozen_step(sz, pf, emb, lat, ctl, zw, ids, *rest)
```
